32 devices in a mesh: gx: 4 (over z), gy: 2 (over y), gz: 4 (over x, core).
Axes of the slice: x: 2, y: 2, z: 4, core: 2. Of those that a mesh axis runs over, the one named last changes fastest.
Arguments:
- atom_x: float32 [4, 8, 256], P('gx', ('gy', 'gz')), may hold values from 0 to 95.99
- atom_y: float32 [4, 8, 256], P('gx', ('gy', 'gz')), may hold values from 0 to 47.99
- atom_z: float32 [4, 8, 256], P('gx', ('gy', 'gz')), may hold values from 0 to 384
- charges: float32 [4, 8, 256], P('gx', ('gy', 'gz')), may hold values from -4.5 to 4.5
- counts: int32 [4, 8], P('gx', ('gy', 'gz')), may hold values from 32 to 256, as said below
- background: float32 [384, 384, 384], P(('gy', 'gz'), 'gx'), may hold values from -0.3125 to 0.3125
Outputs:
- forces: float32 [3, 4, 8, 256], P(None, 'gx', ('gy', 'gz'))
The draws below stay inside these ranges and needn't reach their ends.
Inputs may be any that keep to these rules, and one draw needn't show every extreme that they name: `counts`: live slots come first in each pencil; some pencil is full in every draw.
All inputs are finite; a program needn't handle non-finite values.
Results may differ from the reference program's by a relative error of at most 0.0003.
Values sent between devices are 32-bit elements; how exact they have to be, the bound alone decides.
No kernel may reach another device: no remote copies, remote signals or barrier semaphores. Data moves between devices by JAX's collectives and lax.ppermute only.
A program may use at most 128 MiB of HBM per device.

```python
import math
import jax
import jax.numpy as jnp
from jax import lax

NX = 384
NY = 384
NZ = 384
SLOTS = 256
PENCIL_X = 4
PENCIL_Y = 8


def draw_counts(key, part):
    key_list = jax.random.split(key, 4)
    extent = (PENCIL_X, PENCIL_Y)
    light_load = jax.random.randint(key_list[0], extent, max(SLOTS // 8, 1), SLOTS // 2 + 1)
    heavy_load = jax.random.randint(key_list[1], extent, SLOTS // 2, SLOTS + 1)
    selector = jax.random.randint(key_list[2], extent, 0, 8)
    loads = jnp.where(selector == 0, heavy_load, light_load).reshape(-1)
    full_pencil = jax.random.randint(key_list[3], (), 0, PENCIL_X * PENCIL_Y)
    loads = loads.at[full_pencil].set(SLOTS)
    return loads.reshape(PENCIL_X, PENCIL_Y).astype(jnp.int32)


def draw_charges(key, part):
    key_list = jax.random.split(key, 3)
    extent = (PENCIL_X, PENCIL_Y, SLOTS)
    values = jnp.clip(jax.random.normal(key_list[2], extent), -4.0, 4.0)
    return values.astype(jnp.float32)


def block_scale(key, shape, shards, smallest, top_value):
    def one(axis_at, blocks):
        draws = jax.random.uniform(jax.random.fold_in(jax.random.fold_in(key, 6), axis_at), (blocks,), jnp.float32, smallest / len(shards), top_value / len(shards))
        return jnp.repeat(jnp.exp(draws), shape[axis_at] // blocks).reshape((-1,) + (1,) * (len(shape) - axis_at - 1))

    level = one(*shards[0])
    for cut in shards[1:]:
        level = level * one(*cut)
    return level


def scatter_about(key, shape, deviation, reach, shards=(), dtype=jnp.bfloat16):
    array = deviation * jax.random.normal(key, shape, jnp.float32)
    if shards:
        array = array * block_scale(key, shape, shards, -0.22, 0.18)
    return jnp.clip(array, -reach, reach).astype(dtype)


def setup_inputs(seed: int = 0) -> dict:
    key_of = jax.random.split(jax.random.key(seed), 7)
    return {
        "atom_x": jnp.clip(95.99 * jax.random.uniform(key_of[0], (PENCIL_X, PENCIL_Y, SLOTS), jnp.float32) ** block_scale(key_of[0], (PENCIL_X, PENCIL_Y, SLOTS), ((0, 4), (1, 8)), -0.2, 0.2), 0.0, 95.99),
        "atom_y": jnp.clip(47.99 * jax.random.uniform(key_of[1], (PENCIL_X, PENCIL_Y, SLOTS), jnp.float32) ** block_scale(key_of[1], (PENCIL_X, PENCIL_Y, SLOTS), ((0, 4), (1, 8)), -0.2, 0.2), 0.0, 47.99),
        "atom_z": jnp.clip(384.0 * jax.random.uniform(key_of[2], (PENCIL_X, PENCIL_Y, SLOTS), jnp.float32) ** block_scale(key_of[2], (PENCIL_X, PENCIL_Y, SLOTS), ((0, 4), (1, 8)), -0.2, 0.2), 0.0, 384.0),
        "charges": draw_charges(jax.random.fold_in(key_of[6], 71), 0),
        "counts": draw_counts(jax.random.fold_in(key_of[6], 71), 0),
        "background": scatter_about(key_of[5], (NY, NX, NZ), 0.05, 0.3125, ((0, 8), (1, 4)), jnp.float32),
    }


COULOMB = 6.5
EWALD_BETA = 1.0
PRECISE = lax.Precision.HIGHEST


def spline(offset):
    distance = jnp.minimum(offset, 5.0 - offset)
    ramp_zero = jax.nn.relu(distance)
    ramp_one = jax.nn.relu(distance - 1.0)
    ramp_two = jax.nn.relu(distance - 2.0)
    cube_zero = ramp_zero * ramp_zero * ramp_zero
    cube_one = ramp_one * ramp_one * ramp_one
    cube_two = ramp_two * ramp_two * ramp_two
    height = (cube_zero * ramp_zero - 5.0 * cube_one * ramp_one + 10.0 * cube_two * ramp_two) / 24.0
    gradient = (cube_zero - 5.0 * cube_one + 10.0 * cube_two) / 6.0
    return height, jnp.where(offset < 2.5, gradient, -gradient)


def weights(coord_x, coord_y, coord_z, cells_x, cells_y, depth):
    edge_x = jnp.arange(cells_x + 4).astype(jnp.float32)
    weight_x, slope_x = spline(coord_x[None, :] - edge_x[:, None] + 4.5)
    edge_y = jnp.arange(cells_y + 4).astype(jnp.float32)
    weight_y, slope_y = spline(coord_y[None, :] - edge_y[:, None] + 4.5)
    planes = jnp.arange(depth).astype(jnp.float32)
    halfway = depth / 2.0
    offset_z = jnp.mod(coord_z[:, None] - planes[None, :] + halfway, float(depth)) - halfway + 2.5
    weight_z, slope_z = spline(offset_z)
    return weight_x, slope_x, weight_y, slope_y, weight_z, slope_z


def deposit(stencil, charge_live):
    weight_x, slope_x, weight_y, slope_y, weight_z, slope_z = stencil
    mixed = weight_y[:, None, :] * weight_x[None, :, :] * charge_live[None, None, :]
    flat = mixed.reshape(-1, charge_live.shape[0])
    spread = jnp.dot(flat, weight_z, precision=PRECISE, preferred_element_type=jnp.float32)
    return spread.reshape(weight_y.shape[0], weight_x.shape[0], weight_z.shape[1])


def pull(potential, stencil, charge_live):
    weight_x, slope_x, weight_y, slope_y, weight_z, slope_z = stencil
    extent_y, extent_x, depth = potential.shape
    flat = potential.reshape(extent_y * extent_x, depth)
    dims = (((1,), (1,)), ((), ()))
    plain = lax.dot_general(flat, weight_z, dims, precision=PRECISE, preferred_element_type=jnp.float32)
    deriv = lax.dot_general(flat, slope_z, dims, precision=PRECISE, preferred_element_type=jnp.float32)
    plain = plain.reshape(extent_y, extent_x, -1)
    deriv = deriv.reshape(extent_y, extent_x, -1)
    along_x = jnp.sum(weight_x[None] * plain, axis=1)
    turned_x = jnp.sum(slope_x[None] * plain, axis=1)
    depth_x = jnp.sum(weight_x[None] * deriv, axis=1)
    force_x = -charge_live * jnp.sum(weight_y * turned_x, axis=0)
    force_y = -charge_live * jnp.sum(slope_y * along_x, axis=0)
    force_z = -charge_live * jnp.sum(weight_y * depth_x, axis=0)
    return jnp.stack([force_x, force_y, force_z])


def modulus(indices, length):
    angles = (2.0 * math.pi / length) * indices.astype(jnp.float32)
    return (230.0 + 152.0 * jnp.cos(angles) + 2.0 * jnp.cos(2.0 * angles)) / 384.0


def frequency(indices, length):
    signed = jnp.where(indices <= length // 2, indices, indices - length)
    return signed.astype(jnp.float32) / length


def influence(wave_z, wave_x, wave_y, depth, width_x, width_y):
    freq_z = frequency(wave_z, depth)
    freq_x = frequency(wave_x, width_x)
    freq_y = frequency(wave_y, width_y)
    square = freq_z[:, None, None] ** 2 + freq_x[None, :, None] ** 2 + freq_y[None, None, :] ** 2
    damping = modulus(wave_z, depth)[:, None, None] * modulus(wave_x, width_x)[None, :, None] * modulus(wave_y, width_y)[None, None, :]
    bounded = jnp.where(square > 0.0, square, 1.0)
    factor = COULOMB / (math.pi * width_x * width_y * depth)
    green = factor * jnp.exp(-((math.pi / EWALD_BETA) ** 2) * square) / (bounded * damping * damping)
    return jnp.where(square > 0.0, green, 0.0)


def reference(atom_x, atom_y, atom_z, charges, counts, background):
    cells_x = NX // PENCIL_X
    cells_y = NY // PENCIL_Y
    pencils = PENCIL_X * PENCIL_Y
    slot_ids = jnp.arange(SLOTS).astype(jnp.int32)
    zero_index = jnp.zeros((), jnp.int32)

    def pencil_data(pencil):
        pencil = pencil.astype(jnp.int32)
        column = pencil // PENCIL_Y
        row_index = pencil % PENCIL_Y
        live = slot_ids < counts[column, row_index]
        charge_live = jnp.where(live, charges[column, row_index], 0.0)
        stencil = weights(atom_x[column, row_index], atom_y[column, row_index], atom_z[column, row_index], cells_x, cells_y, NZ)
        return column, row_index, charge_live, stencil

    def add_pencil(pencil, padded):
        column, row_index, charge_live, stencil = pencil_data(pencil)
        spread = deposit(stencil, charge_live)
        start_y = (row_index * cells_y).astype(jnp.int32)
        start_x = (column * cells_x).astype(jnp.int32)
        current = lax.dynamic_slice(padded, (start_y, start_x, zero_index), spread.shape)
        return lax.dynamic_update_slice(padded, current + spread, (start_y, start_x, zero_index))

    padded = lax.fori_loop(0, pencils, add_pencil, jnp.zeros((NY + 4, NX + 4, NZ), jnp.float32))
    rows_done = padded[2:NY + 2]
    rows_done = rows_done.at[:2].add(padded[NY + 2:]).at[NY - 2:].add(padded[:2])
    charge_grid = rows_done[:, 2:NX + 2]
    charge_grid = charge_grid.at[:, :2].add(rows_done[:, NX + 2:]).at[:, NX - 2:].add(rows_done[:, :2])
    charge_grid = charge_grid + background
    spectrum = jnp.fft.fftn(charge_grid)
    green = influence(jnp.arange(NZ).astype(jnp.int32), jnp.arange(NX).astype(jnp.int32), jnp.arange(NY).astype(jnp.int32), NZ, NX, NY)
    green = jnp.transpose(green, (2, 1, 0))
    potential = jnp.real(jnp.fft.ifftn(spectrum * green)) * float(NX * NY * NZ)
    wrapped = jnp.pad(potential, ((2, 2), (2, 2), (0, 0)), mode="wrap")

    def gather_pencil(pencil):
        column, row_index, charge_live, stencil = pencil_data(pencil)
        start_y = (row_index * cells_y).astype(jnp.int32)
        start_x = (column * cells_x).astype(jnp.int32)
        local = lax.dynamic_slice(wrapped, (start_y, start_x, zero_index), (cells_y + 4, cells_x + 4, NZ))
        return pull(local, stencil, charge_live)

    forces = lax.map(gather_pencil, jnp.arange(pencils).astype(jnp.int32))
    return forces.reshape(PENCIL_X, PENCIL_Y, 3, SLOTS).transpose(2, 0, 1, 3)
```

```python
import functools
import math

import jax
import jax.numpy as jnp
from jax import lax
from jax.experimental import pallas as pl
from jax.experimental.pallas import tpu as pltpu
from jax.sharding import PartitionSpec as P

COULOMB = 6.5
EWALD_BETA = 1.0
PRECISE = lax.Precision.HIGHEST
PAD = 8
PLANE = ("gy", "gz")


def spline(offset):
    distance = jnp.minimum(offset, 5.0 - offset)
    ramp_zero = jax.nn.relu(distance)
    ramp_one = jax.nn.relu(distance - 1.0)
    ramp_two = jax.nn.relu(distance - 2.0)
    cube_zero = ramp_zero * ramp_zero * ramp_zero
    cube_one = ramp_one * ramp_one * ramp_one
    cube_two = ramp_two * ramp_two * ramp_two
    height = (cube_zero * ramp_zero - 5.0 * cube_one * ramp_one + 10.0 * cube_two * ramp_two) / 24.0
    gradient = (cube_zero - 5.0 * cube_one + 10.0 * cube_two) / 6.0
    return (height, jnp.where(offset < 2.5, gradient, -gradient))


def cas_table(rows, cols, length):
    angles = jnp.mod(rows[:, None] * cols[None, :], length).astype(jnp.float32) * (
        2.0 * math.pi / length
    )
    return jnp.cos(angles) + jnp.sin(angles)


def modulus(indices, length):
    angles = 2.0 * math.pi / length * indices.astype(jnp.float32)
    return (230.0 + 152.0 * jnp.cos(angles) + 2.0 * jnp.cos(2.0 * angles)) / 384.0


def axis_factors(indices, length):
    signed = jnp.where(indices <= length // 2, indices, indices - length)
    square = (signed.astype(jnp.float32) / length) ** 2
    damping = modulus(indices, length)
    return square, jnp.exp(-((math.pi / EWALD_BETA) ** 2) * square) / (damping * damping)


def halves(value):
    high = value.astype(jnp.bfloat16)
    return high, (value - high.astype(jnp.float32)).astype(jnp.bfloat16)


def product(left, right, dims=(((1,), (0,)), ((), ()))):
    dot = functools.partial(
        lax.dot_general, dimension_numbers=dims, preferred_element_type=jnp.float32
    )
    left_high, left_low = left
    right_high, right_low = right
    return dot(left_high, right_high) + (dot(left_low, right_high) + dot(left_high, right_low))


NT = (((1,), (1,)), ((), ()))


def depth_kernel(grid_ref, table_ref, out_ref):
    rows, cells_x, depth = grid_ref.shape
    parts = out_ref.shape[0]
    strip = table_ref.shape[1] // parts
    block = grid_ref[...].reshape(rows * cells_x, depth)
    table = halves(table_ref[...])
    moved = product(halves(block), table)
    for part in range(parts):
        for row in range(rows):
            out_ref[part, 0, :, row * strip : (row + 1) * strip] = moved[
                row * cells_x : (row + 1) * cells_x, part * strip : (part + 1) * strip
            ]


def depth_stage(background, table, parts, rows):
    cells_y, cells_x, depth = background.shape
    strip = table.shape[1] // parts
    groups = cells_y // rows
    return pl.pallas_call(
        depth_kernel,
        grid=(groups,),
        in_specs=[
            pl.BlockSpec((rows, cells_x, depth), lambda g: (g, 0, 0)),
            pl.BlockSpec(table.shape, lambda g: (0, 0)),
        ],
        out_specs=pl.BlockSpec((parts, 1, cells_x, rows * strip), lambda g: (0, g, 0, 0)),
        out_shape=jax.ShapeDtypeStruct((parts, groups, cells_x, rows * strip), jnp.float32),
        name="depth_stage",
    )(background, table)


def deposit_kernel(wx_ref, wy_ref, bz_ref, *refs):
    count = len(refs) // 2
    out_refs, ext_refs = refs[:count], refs[count:]
    parts, window, slots = wx_ref.shape
    strip = bz_ref.shape[1] // count
    rows = wy_ref.shape[1] // parts
    width = out_refs[0].shape[1]
    step = width // parts
    for ext_ref in ext_refs:
        ext_ref[...] = jnp.zeros_like(ext_ref)
    for part in range(parts):
        bz = halves(bz_ref[part])
        wx = wx_ref[part]
        for row in range(rows):
            wy = wy_ref[0, row * parts + part : row * parts + part + 1, :]
            spread = product(halves(wx * wy), bz, NT)
            for chunk, ext_ref in enumerate(ext_refs):
                ext_ref[part * step : part * step + window, row * strip : (row + 1) * strip] += (
                    spread[:, chunk * strip : (chunk + 1) * strip]
                )
    for out_ref, ext_ref in zip(out_refs, ext_refs):
        out_ref[0] = ext_ref[PAD : PAD + width]
        out_ref[0, width - PAD :] += ext_ref[:PAD]
        out_ref[0, :PAD] += ext_ref[PAD + width :]


def deposit_stage(weight_x, weight_y, charged, width, count):
    parts, window, slots = weight_x.shape
    groups, flat, _ = weight_y.shape
    strip = charged.shape[1]
    lanes = flat // parts * (strip // count)
    return pl.pallas_call(
        deposit_kernel,
        grid=(groups,),
        in_specs=[
            pl.BlockSpec((parts, window, slots), lambda g: (0, 0, 0)),
            pl.BlockSpec((1, flat, slots), lambda g: (g, 0, 0)),
            pl.BlockSpec((parts, strip, slots), lambda g: (0, 0, 0)),
        ],
        out_specs=[pl.BlockSpec((1, width, lanes), lambda g: (g, 0, 0))] * count,
        out_shape=[jax.ShapeDtypeStruct((groups, width, lanes), jnp.float32)] * count,
        scratch_shapes=[pltpu.VMEM((width + 2 * PAD, lanes), jnp.float32)] * count,
        name="deposit_stage",
    )(weight_x, weight_y, charged)


def cross_kernel(grid_ref, spread_ref, low_ref, high_ref, table_ref, *out_refs):
    width = table_ref.shape[0]
    lanes = grid_ref.shape[-1]
    group = pl.program_id(0)
    first = (group == 0).astype(jnp.float32)
    last = (group == pl.num_programs(0) - 1).astype(jnp.float32)
    block = grid_ref[...].reshape(width, lanes) + spread_ref[0]
    block = block + first * low_ref[...] + last * high_ref[...]
    moved = product(halves(table_ref[...]), halves(block))
    strip = width // len(out_refs)
    for peer, out_ref in enumerate(out_refs):
        out_ref[0] = moved[peer * strip : (peer + 1) * strip]


def cross_stage(received, spread, low, high, table, parts_y):
    parts, groups, cells_x, lanes = received.shape
    width = parts * cells_x
    strip = width // parts_y
    return pl.pallas_call(
        cross_kernel,
        grid=(groups,),
        in_specs=[
            pl.BlockSpec((parts, 1, cells_x, lanes), lambda g: (0, g, 0, 0)),
            pl.BlockSpec((1, width, lanes), lambda g: (g, 0, 0)),
            pl.BlockSpec((width, lanes), lambda g: (0, 0)),
            pl.BlockSpec((width, lanes), lambda g: (0, 0)),
            pl.BlockSpec((width, width), lambda g: (0, 0)),
        ],
        out_specs=[pl.BlockSpec((1, strip, lanes), lambda g: (g, 0, 0))] * parts_y,
        out_shape=[jax.ShapeDtypeStruct((groups, strip, lanes), jnp.float32)] * parts_y,
        name="cross_stage",
    )(received, spread, low, high, table)


def solve_kernel(parts, *refs):
    lines_refs = refs[:parts]
    ahead_ref, back_ref, square_y_ref, factor_y_ref, square_ref, factor_ref = refs[parts : parts + 6]
    out_refs, block_ref = refs[parts + 6 : -1], refs[-1]
    groups, step, lanes = lines_refs[0].shape
    beyond = out_refs[0].shape[0]
    width = ahead_ref.shape[1]
    rows = width // (parts * groups)
    strip = lanes // rows
    near = parts * groups
    far = parts * beyond
    for wave in range(step):
        held = jnp.concatenate([ref[:, wave, :] for ref in lines_refs], axis=0)
        for row in range(rows):
            block_ref[row * near : (row + 1) * near, wave * strip : (wave + 1) * strip] = held[
                :, row * strip : (row + 1) * strip
            ]
    modes = product(halves(ahead_ref[...]), halves(block_ref[...]))
    square = square_y_ref[...] + square_ref[0]
    bounded = jnp.where(square > 0.0, square, 1.0)
    green = factor_y_ref[...] * factor_ref[0] / bounded
    modes = jnp.where(square > 0.0, modes * green, 0.0)
    field = product(halves(back_ref[...]), halves(modes))
    for wave in range(step):
        held = jnp.concatenate(
            [
                field[row * far : (row + 1) * far, wave * strip : (wave + 1) * strip]
                for row in range(rows)
            ],
            axis=1,
        )
        for peer, out_ref in enumerate(out_refs):
            out_ref[:, wave, :] = held[peer * beyond : (peer + 1) * beyond]


def solve_stage(lines, ahead, back, square_y, factor_y, square, factor):
    parts = len(lines)
    groups, strip_x, lanes = lines[0].shape
    width = ahead.shape[0]
    extent = back.shape[0]
    beyond = groups + 1
    count = square.shape[0]
    step = strip_x // count
    waves = square.shape[-1]
    return pl.pallas_call(
        functools.partial(solve_kernel, parts),
        grid=(count,),
        in_specs=[pl.BlockSpec((groups, step, lanes), lambda g: (0, g, 0))] * parts
        + [
            pl.BlockSpec((width, width), lambda g: (0, 0)),
            pl.BlockSpec((extent, width), lambda g: (0, 0)),
            pl.BlockSpec((width, 1), lambda g: (0, 0)),
            pl.BlockSpec((width, 1), lambda g: (0, 0)),
            pl.BlockSpec((1, 1, waves), lambda g: (g, 0, 0)),
            pl.BlockSpec((1, 1, waves), lambda g: (g, 0, 0)),
        ],
        out_specs=[pl.BlockSpec((beyond, step, lanes), lambda g: (0, g, 0))] * parts,
        out_shape=[jax.ShapeDtypeStruct((beyond, strip_x, lanes), jnp.float32)] * parts,
        scratch_shapes=[pltpu.VMEM((width, waves), jnp.float32)],
        name="solve_stage",
    )(*lines, ahead, back, square_y, factor_y, square, factor)


def pull_kernel(count, *refs):
    lines_refs = refs[:count]
    table_ref, wx_ref, sx_ref, wy_ref, sy_ref, bz_ref, out_ref, left_ref, right_ref = refs[count:]
    parts, window, slots = wx_ref.shape
    strip = bz_ref.shape[1]
    rows = wy_ref.shape[1] // parts
    width = table_ref.shape[0]
    step = width // parts

    @pl.when(pl.program_id(0) == 0)
    def _():
        out_ref[...] = jnp.zeros_like(out_ref)
        for part in range(parts):
            high, low = halves(bz_ref[part])
            right_ref[part] = jnp.concatenate([high, high, low], axis=0)

    block = jnp.concatenate([ref[0] for ref in lines_refs], axis=0)
    field = product(halves(table_ref[...]), halves(block))
    for row in range(rows):
        local = field[:, row * strip : (row + 1) * strip]
        local = jnp.concatenate([local[width - PAD :], local, local[:PAD]], axis=0)
        high, low = halves(local)
        left_ref[row] = jnp.concatenate([high, low, high], axis=1)
    for part in range(parts):
        right = right_ref[part]
        wx = wx_ref[part]
        sx = sx_ref[part]
        force_x = jnp.zeros((1, slots), jnp.float32)
        force_y = jnp.zeros((1, slots), jnp.float32)
        force_z = jnp.zeros((1, slots), jnp.float32)
        for row in range(rows):
            both = jnp.dot(
                left_ref[row, part * step : part * step + window],
                right,
                preferred_element_type=jnp.float32,
            )
            plain = both[:, :slots]
            deriv = both[:, slots:]
            at = slice(row * parts + part, row * parts + part + 1)
            wy = wy_ref[0, at, :]
            sy = sy_ref[0, at, :]
            force_x += wy * jnp.sum(sx * plain, axis=0, keepdims=True)
            force_y += sy * jnp.sum(wx * plain, axis=0, keepdims=True)
            force_z += wy * jnp.sum(wx * deriv, axis=0, keepdims=True)
        out_ref[part, 0:1] += force_x
        out_ref[part, 1:2] += force_y
        out_ref[part, 2:3] += force_z


def pull_stage(lines, table, weight_x, slope_x, weight_y, slope_y, depth_pair):
    parts_y = len(lines)
    groups, strip_x, lanes = lines[0].shape
    width = parts_y * strip_x
    parts, window, slots = weight_x.shape
    flat = weight_y.shape[1]
    strip = depth_pair.shape[1]
    return pl.pallas_call(
        functools.partial(pull_kernel, parts_y),
        grid=(groups,),
        in_specs=[pl.BlockSpec((1, strip_x, lanes), lambda g: (g, 0, 0))] * parts_y
        + [
            pl.BlockSpec((width, width), lambda g: (0, 0)),
            pl.BlockSpec((parts, window, slots), lambda g: (0, 0, 0)),
            pl.BlockSpec((parts, window, slots), lambda g: (0, 0, 0)),
            pl.BlockSpec((1, flat, slots), lambda g: (g, 0, 0)),
            pl.BlockSpec((1, flat, slots), lambda g: (g, 0, 0)),
            pl.BlockSpec((parts, strip, 2 * slots), lambda g: (0, 0, 0)),
        ],
        out_specs=pl.BlockSpec((parts, 8, slots), lambda g: (0, 0, 0)),
        out_shape=jax.ShapeDtypeStruct((parts, 8, slots), jnp.float32),
        scratch_shapes=[
            pltpu.VMEM((flat // parts, width + 2 * PAD, 3 * strip), jnp.bfloat16),
            pltpu.VMEM((parts, 3 * strip, 2 * slots), jnp.bfloat16),
        ],
        name="pull_stage",
    )(*lines, table, weight_x, slope_x, weight_y, slope_y, depth_pair)


def depth_plain(background, table, parts, rows):
    cells_y, cells_x, depth = background.shape
    moved = jnp.einsum("yxz,zk->yxk", background, table, precision=PRECISE)
    moved = moved.reshape(cells_y // rows, rows, cells_x, parts, -1)
    return moved.transpose(3, 0, 2, 1, 4).reshape(parts, cells_y // rows, cells_x, -1)


def deposit_plain(weight_x, weight_y, charged, width, count):
    size = charged.shape[1] // count
    return [
        deposit_one(weight_x, weight_y, charged[:, i * size : (i + 1) * size], width)
        for i in range(count)
    ]


def deposit_one(weight_x, weight_y, charged, width):
    parts, window, slots = weight_x.shape
    groups, flat, _ = weight_y.shape
    wy = weight_y.reshape(groups, flat // parts, parts, slots)
    spread = jnp.einsum("pxa,grpa,pka->gpxrk", weight_x, wy, charged, precision=PRECISE)
    spread = spread.reshape(groups, parts, window, -1)
    step = width // parts
    total = jnp.zeros((groups, width, spread.shape[-1]), jnp.float32)
    for part in range(parts):
        place = jnp.mod(part * step - PAD + jnp.arange(window), width)
        total = total.at[:, place].add(spread[:, part])
    return total


def cross_plain(received, spread, low, high, table, parts_y):
    parts, groups, cells_x, lanes = received.shape
    spread = spread[:groups].at[0].add(low).at[groups - 1].add(high)
    block = received.transpose(1, 0, 2, 3).reshape(groups, parts * cells_x, lanes) + spread
    moved = jnp.einsum("kx,gxl->gkl", table, block, precision=PRECISE)
    moved = moved.reshape(groups, parts_y, -1, lanes)
    return [moved[:, i] for i in range(parts_y)]


def solve_plain(lines, ahead, back, square_y, factor_y, square, factor):
    lines = jnp.stack(lines)
    parts, groups, strip_x, lanes = lines.shape
    width = ahead.shape[0]
    rows = width // (parts * groups)
    lines = lines.reshape(parts, groups, strip_x, rows, -1).transpose(3, 0, 1, 2, 4)
    modes = jnp.dot(ahead, lines.reshape(width, -1), precision=PRECISE)
    total = square_y + square.reshape(1, -1)
    bounded = jnp.where(total > 0.0, total, 1.0)
    green = jnp.where(total > 0.0, factor_y * factor.reshape(1, -1) / bounded, 0.0)
    field = jnp.dot(back, modes * green, precision=PRECISE)
    field = field.reshape(rows, parts, groups + 1, strip_x, -1).transpose(1, 2, 3, 0, 4)
    field = field.reshape(parts, groups + 1, strip_x, lanes)
    return [field[i] for i in range(parts)]


def pull_plain(lines, table, weight_x, slope_x, weight_y, slope_y, depth_pair):
    lines = jnp.stack(lines)
    parts_y, groups, strip_x, lanes = lines.shape
    width = parts_y * strip_x
    parts, window, slots = weight_x.shape
    strip = depth_pair.shape[1]
    block = lines.transpose(1, 0, 2, 3).reshape(groups, width, lanes)
    field = jnp.einsum("xk,gkl->gxl", table, block, precision=PRECISE)
    field = field.reshape(groups, width, lanes // strip, strip)
    step = width // parts
    wy = weight_y.reshape(groups, -1, parts, slots)
    sy = slope_y.reshape(groups, -1, parts, slots)
    out = []
    for part in range(parts):
        place = jnp.mod(part * step - PAD + jnp.arange(window), width)
        both = jnp.einsum("gxrk,ka->gxra", field[:, place], depth_pair[part], precision=PRECISE)
        plain = both[..., :slots]
        deriv = both[..., slots:]
        wx = weight_x[part][None, :, None, :]
        sx = slope_x[part][None, :, None, :]
        out.append(
            jnp.stack(
                [
                    jnp.sum(wy[:, :, part] * jnp.sum(sx * plain, axis=1), axis=(0, 1)),
                    jnp.sum(sy[:, :, part] * jnp.sum(wx * plain, axis=1), axis=(0, 1)),
                    jnp.sum(wy[:, :, part] * jnp.sum(wx * deriv, axis=1), axis=(0, 1)),
                ]
            )
        )
    return jnp.pad(jnp.stack(out), ((0, 0), (0, 5), (0, 0)))


def ring(axis, step):
    count = lax.axis_size(axis)
    return [(i, (i + step) % count) for i in range(count)]


def partner(index, step, count):
    if count & (count - 1) == 0:
        return index ^ step, index ^ step
    return (index + step) % count, (index - step) % count


def targets(index, count):
    return jnp.stack([partner(index, step, count)[0] for step in range(count)])


def sources(index, count):
    return jnp.stack([partner(index, step, count)[1] for step in range(count)])


def exchange(blocks, axis):
    count = len(blocks)
    got = [blocks[0]]
    for step in range(1, count):
        pairs = [(i, partner(i, step, count)[0]) for i in range(count)]
        got.append(lax.ppermute(blocks[step], axis, pairs))
    return got


CHUNKS = 2


def per_device(atom_x, atom_y, atom_z, charges, counts, background):
    slots = atom_x.shape[-1]
    cells_y, cells_x, depth = background.shape
    parts_x = lax.axis_size("gx")
    parts_y = lax.axis_size(PLANE)
    width_x = cells_x * parts_x
    width_y = cells_y * parts_y
    strip_z = depth // parts_x
    strip_x = width_x // parts_y
    part_z = strip_z // CHUNKS
    rows = next(
        (r for r in range(4, cells_y) if cells_y % r == 0 and r * part_z % 128 == 0), cells_y
    )
    groups = cells_y // rows
    lanes = rows * part_z
    tiled = lanes % 128 == 0 and cells_x % 8 == 0 and strip_x % 8 == 0 and part_z % 16 == 0
    if tiled:
        depth_do, deposit_do, cross_do, solve_do, pull_do = (
            depth_stage, deposit_stage, cross_stage, solve_stage, pull_stage
        )
    else:
        depth_do, deposit_do, cross_do, solve_do, pull_do = (
            depth_plain, deposit_plain, cross_plain, solve_plain, pull_plain
        )

    live = jnp.arange(slots) < counts.reshape(())
    charge_live = jnp.where(live, charges.reshape(slots), 0.0)
    own = jnp.stack(
        [atom_x.reshape(slots), atom_y.reshape(slots), atom_z.reshape(slots), charge_live]
    )
    place_x = lax.axis_index("gx")
    place_y = lax.axis_index(PLANE)
    gathered = jnp.stack(exchange([own] * parts_x, "gx"))
    slot_of = jnp.argsort(sources(place_x, parts_x))
    atoms = jnp.stack(
        [lax.dynamic_index_in_dim(gathered, slot_of[i], 0, False) for i in range(parts_x)]
    )

    starts = jnp.arange(parts_x)[:, None] * strip_z + jnp.arange(part_z)
    order = jnp.concatenate([(starts + i * part_z).reshape(-1) for i in range(CHUNKS)])
    table_z = cas_table(jnp.arange(depth), order, depth)
    span = parts_x * part_z
    sent = depth_do(background, table_z[:, :span], parts_x, rows)
    sent, atoms = lax.optimization_barrier((sent, atoms))
    received = [lax.all_to_all(sent, "gx", split_axis=0, concat_axis=0, tiled=True)]

    modes_z = lax.axis_index("gx") * strip_z + jnp.arange(strip_z)
    modes_x = lax.axis_index(PLANE) * strip_x + jnp.arange(strip_x)
    cells_all = jnp.arange(width_x)
    strips = jnp.arange(strip_x)
    sent_x = (targets(place_y, parts_y)[:, None] * strip_x + strips).reshape(-1)
    came_x = (sources(place_y, parts_y)[:, None] * strip_x + strips).reshape(-1)
    table_x = cas_table(sent_x, cells_all, width_x)
    table_back_x = cas_table(cells_all, came_x, width_x)
    window = cells_x + 2 * PAD
    edge_x = (jnp.arange(window) - PAD).astype(jnp.float32)
    within = ((edge_x >= -2.0) & (edge_x < cells_x + 2.0))[None, :, None]
    weight_x, slope_x = (
        jnp.where(within, part, 0.0)
        for part in spline(atoms[:, 0, None, :] - edge_x[None, :, None] + 2.5)
    )
    inner = jnp.arange(cells_y)
    outer = jnp.concatenate(
        [
            jnp.array([-2, -1, cells_y, cells_y + 1]),
            jnp.full((rows - 4,), -100 * cells_y, inner.dtype),
        ]
    )
    edge_y = jnp.concatenate([inner, outer]).astype(jnp.float32)
    weight_y, slope_y = spline(atoms[None, :, 1, :] - edge_y[:, None, None] + 2.5)
    weight_y = weight_y.reshape(groups + 1, rows * parts_x, slots)
    slope_y = slope_y.reshape(groups + 1, rows * parts_x, slots)
    planes = jnp.arange(depth).astype(jnp.float32)
    halfway = depth / 2.0
    coord_z = atoms[:, 2, :].reshape(1, -1)
    offset_z = coord_z - planes[:, None]
    offset_z = jnp.where(offset_z < -halfway, offset_z + depth, offset_z)
    offset_z = jnp.where(offset_z >= halfway, offset_z - depth, offset_z)
    splines_z = jnp.concatenate(spline(offset_z + 2.5), axis=1)
    table_strip = cas_table(modes_z, jnp.arange(depth), depth)
    pair = jnp.dot(table_strip, splines_z, precision=PRECISE).reshape(
        strip_z, 2, parts_x, slots
    )
    depth_pair = pair.transpose(2, 0, 1, 3).reshape(parts_x, strip_z, 2 * slots)
    charged = depth_pair[:, :, :slots] * atoms[:, 3, None, :]
    spreads = deposit_do(weight_x, weight_y, charged, width_x, CHUNKS)
    half = 2 * part_z
    beyond = jnp.concatenate([spread[groups, :, : 2 * half] for spread in spreads], axis=1)
    beyond = beyond.reshape(width_x, CHUNKS, 2, half)
    low = lax.ppermute(beyond[:, :, 1].reshape(width_x, -1), PLANE, ring(PLANE, 1))
    high = lax.ppermute(beyond[:, :, 0].reshape(width_x, -1), PLANE, ring(PLANE, -1))
    table_z, low, high = lax.optimization_barrier((table_z, low, high))
    for i in range(1, CHUNKS):
        sent = depth_do(background, table_z[:, i * span : (i + 1) * span], parts_x, rows)
        received.append(lax.all_to_all(sent, "gx", split_axis=0, concat_axis=0, tiled=True))

    near = (
        jnp.arange(rows)[:, None, None]
        + sources(place_y, parts_y)[None, :, None] * cells_y
        + jnp.arange(groups)[None, None, :] * rows
    )
    sent_y = (
        jnp.arange(rows)[:, None, None]
        + targets(place_y, parts_y)[None, :, None] * cells_y
        + jnp.arange(groups)[None, None, :] * rows
    )
    far = jnp.broadcast_to(
        jnp.where(outer < -cells_y, 0, outer)[:, None, None]
        + targets(place_y, parts_y)[None, :, None] * cells_y,
        (rows, parts_y, 1),
    )
    modes_y = jnp.arange(width_y)
    ahead = cas_table(modes_y, near.reshape(-1), width_y)
    cells = jnp.mod(jnp.concatenate([sent_y, far], axis=2).reshape(-1), width_y)
    back = cas_table(cells, modes_y, width_y)
    square_y, factor_y = axis_factors(modes_y, width_y)
    square_x, factor_x = axis_factors(modes_x, width_x)
    square_z, factor_z = axis_factors(modes_z, depth)
    scale = COULOMB / (math.pi * width_x * width_y * depth)
    step = 8 if tiled else strip_x

    wave_lines = []
    for i in range(CHUNKS):
        mine = slice(i * half, (i + 1) * half)
        below = jnp.pad(low[:, mine], ((0, 0), (0, lanes - half)))
        above = jnp.pad(high[:, mine], ((0, 0), (lanes - half, 0)))
        columns = cross_do(received[i], spreads[i], below, above, table_x, parts_y)
        wave_lines.append(exchange(columns, PLANE))
    returned = []
    for i in range(CHUNKS):
        at = slice(i * part_z, (i + 1) * part_z)
        square = (square_x[:, None] + square_z[None, at]).reshape(strip_x // step, 1, -1)
        factor = (scale * factor_x[:, None] * factor_z[None, at]).reshape(square.shape)
        solved = solve_do(
            wave_lines[i], ahead, back, square_y[:, None], factor_y[:, None], square, factor
        )
        returned.append(exchange(solved, PLANE))
    partial = 0.0
    for i in range(CHUNKS):
        at = slice(i * part_z, (i + 1) * part_z)
        partial += pull_do(
            returned[i], table_back_x, weight_x, slope_x, weight_y, slope_y, depth_pair[:, at]
        )
    shares = lax.all_to_all(partial, "gx", split_axis=0, concat_axis=0, tiled=True)
    forces = -charge_live * jnp.sum(shares, axis=0)[:3]
    return forces.reshape(3, 1, 1, slots)


def solution(mesh):
    in_specs = (
        P("gx", PLANE, None),
        P("gx", PLANE, None),
        P("gx", PLANE, None),
        P("gx", PLANE, None),
        P("gx", PLANE),
        P(PLANE, "gx", None),
    )
    out_specs = P(None, "gx", PLANE, None)
    return jax.shard_map(
        per_device,
        mesh=mesh,
        in_specs=in_specs,
        out_specs=out_specs,
        check_vma=False,
    )
```

```python
import functools
import math

import jax
import jax.numpy as jnp
from jax import lax
from jax.experimental import pallas as pl
from jax.experimental.pallas import tpu as pltpu
from jax.sharding import PartitionSpec as P


COULOMB = 6.5
EWALD_BETA = 1.0
PRECISE = lax.Precision.HIGHEST
PAD = 8
PLANE = ("gy", "gz")


def spline(offset):
    distance = jnp.minimum(offset, 5.0 - offset)
    ramp_zero = jax.nn.relu(distance)
    ramp_one = jax.nn.relu(distance - 1.0)
    ramp_two = jax.nn.relu(distance - 2.0)
    cube_zero = ramp_zero * ramp_zero * ramp_zero
    cube_one = ramp_one * ramp_one * ramp_one
    cube_two = ramp_two * ramp_two * ramp_two
    height = (cube_zero * ramp_zero - 5.0 * cube_one * ramp_one + 10.0 * cube_two * ramp_two) / 24.0
    gradient = (cube_zero - 5.0 * cube_one + 10.0 * cube_two) / 6.0
    return (height, jnp.where(offset < 2.5, gradient, -gradient))


def cas_table(rows, cols, length):
    angles = jnp.mod(rows[:, None] * cols[None, :], length).astype(jnp.float32) * (
        2.0 * math.pi / length
    )
    return math.sqrt(2.0) * jnp.sin(angles + math.pi / 4.0)


def modulus(indices, length):
    angles = 2.0 * math.pi / length * indices.astype(jnp.float32)
    return (230.0 + 152.0 * jnp.cos(angles) + 2.0 * jnp.cos(2.0 * angles)) / 384.0


def axis_factors(indices, length):
    signed = jnp.where(indices <= length // 2, indices, indices - length)
    square = (signed.astype(jnp.float32) / length) ** 2
    damping = modulus(indices, length)
    return square, jnp.exp(-((math.pi / EWALD_BETA) ** 2) * square) / (damping * damping)


def halves(value):
    high = value.astype(jnp.bfloat16)
    return high, (value - high.astype(jnp.float32)).astype(jnp.bfloat16)


def product(left, right):
    left_high, left_low = left
    right_high, right_low = right
    return jnp.dot(
        jnp.concatenate([left_high, left_low, left_high], axis=1),
        jnp.concatenate([right_high, right_high, right_low], axis=0),
        preferred_element_type=jnp.float32,
    )


def turned_product(left, right):
    left_high, left_low = left
    right_high, right_low = right
    return lax.dot_general(
        jnp.concatenate([left_high, left_low, left_high], axis=1),
        jnp.concatenate([right_high, right_high, right_low], axis=1),
        (((1,), (1,)), ((), ())),
        preferred_element_type=jnp.float32,
    )


def narrow_product(left, right):
    left_high, left_low = left
    right_high, right_low = right
    count = right_high.shape[1]
    dot = functools.partial(jnp.dot, preferred_element_type=jnp.float32)
    both = dot(left_high, jnp.concatenate([right_high, right_low], axis=1))
    return both[:, :count] + (both[:, count:] + dot(left_low, right_high))


def basis_kernel(
    atoms_ref, table_ref, wx_ref, sx_ref, wy_ref, sy_ref, bz_ref, bq_ref, *, cells_x, cells_y
):
    parts, window, slots = wx_ref.shape
    beyond, flat, _ = wy_ref.shape
    rows = flat // parts
    depth = table_ref.shape[1]
    table = halves(table_ref[...])
    edge_x = lax.broadcasted_iota(jnp.int32, (window, slots), 0).astype(jnp.float32) - PAD
    within = (edge_x >= -2.0) & (edge_x < cells_x + 2.0)
    planes = lax.broadcasted_iota(jnp.int32, (depth, slots), 0).astype(jnp.float32)
    halfway = depth / 2.0
    for part in range(parts):
        height, gradient = spline(atoms_ref[part, 0:1, :] - edge_x + 2.5)
        wx_ref[part] = jnp.where(within, height, 0.0)
        sx_ref[part] = jnp.where(within, gradient, 0.0)
        offset = atoms_ref[part, 2:3, :] - planes
        offset = jnp.where(offset < -halfway, offset + depth, offset)
        offset = jnp.where(offset >= halfway, offset - depth, offset)
        both = jnp.concatenate(spline(offset + 2.5), axis=1)
        waves = product(table, halves(both))
        bz_ref[:, part * 2 * slots : (part + 1) * 2 * slots] = waves
        bq_ref[:, part * slots : (part + 1) * slots] = waves[:, :slots] * atoms_ref[part, 3:4, :]
    edges = list(range(cells_y)) + [-2, -1, cells_y, cells_y + 1]
    coord = jnp.concatenate([atoms_ref[part, 1:2, :] for part in range(parts)], axis=0)
    for group in range(beyond):
        inside = [coord - float(edges[group * rows + row]) for row in range(rows)]
        height, gradient = spline(jnp.concatenate(inside, axis=0) + 2.5)
        wy_ref[group] = height
        sy_ref[group] = gradient


def basis_stage(atoms, table, cells_x, cells_y, rows):
    parts, _, slots = atoms.shape
    strip = table.shape[0]
    window = cells_x + 2 * PAD
    weight_x = jax.ShapeDtypeStruct((parts, window, slots), jnp.float32)
    weight_y = jax.ShapeDtypeStruct((cells_y // rows + 1, rows * parts, slots), jnp.float32)
    return pl.pallas_call(
        functools.partial(basis_kernel, cells_x=cells_x, cells_y=cells_y),
        out_shape=[
            weight_x,
            weight_x,
            weight_y,
            weight_y,
            jax.ShapeDtypeStruct((strip, parts * 2 * slots), jnp.float32),
            jax.ShapeDtypeStruct((strip, parts * slots), jnp.float32),
        ],
        name="basis_stage",
    )(atoms, table)


def depth_kernel(grid_ref, table_ref, _, *out_refs):
    total, cells_x, depth = grid_ref.shape
    parts = len(out_refs)
    strip = table_ref.shape[1] // parts
    batch = out_refs[0].shape[0]
    rows = total // batch
    block = grid_ref[...].reshape(total * cells_x, depth)
    table = halves(table_ref[...])
    multiply = narrow_product if table_ref.shape[1] == 128 else product
    moved = multiply(halves(block), table)
    for part, out_ref in enumerate(out_refs):
        for group in range(batch):
            for row in range(rows):
                at = (group * rows + row) * cells_x
                out_ref[group, :, row * strip : (row + 1) * strip] = moved[
                    at : at + cells_x, part * strip : (part + 1) * strip
                ]


def depth_stage(background, table, parts, rows, after):
    cells_y, cells_x, depth = background.shape
    strip = table.shape[1] // parts
    groups = cells_y // rows
    batch = 3 if groups % 3 == 0 else 1
    return pl.pallas_call(
        depth_kernel,
        grid=(groups // batch,),
        in_specs=[
            pl.BlockSpec((batch * rows, cells_x, depth), lambda g: (g, 0, 0)),
            pl.BlockSpec(table.shape, lambda g: (0, 0)),
            pl.BlockSpec(memory_space=pl.ANY),
        ],
        out_specs=[pl.BlockSpec((batch, cells_x, rows * strip), lambda g: (g, 0, 0))] * parts,
        out_shape=[jax.ShapeDtypeStruct((groups, cells_x, rows * strip), jnp.float32)] * parts,
        name="depth_stage",
    )(background, table, after)


def deposit_kernel(wx_ref, wy_ref, bq_ref, *refs):
    count = (len(refs) - 2) // 2
    out_refs, low_ref, high_ref, ext_refs = refs[:count], refs[count], refs[count + 1], refs[count + 2 :]
    parts, window, slots = wx_ref.shape
    strip = bq_ref.shape[0] // count
    half = 2 * strip
    rows = wy_ref.shape[1] // parts
    width = out_refs[0].shape[1]
    step = width // parts
    for ext_ref in ext_refs:
        ext_ref[...] = jnp.zeros_like(ext_ref)
    for part in range(parts):
        bq = halves(bq_ref[:, part * slots : (part + 1) * slots])
        wx = wx_ref[part]
        for row in range(rows):
            wy = wy_ref[0, row * parts + part : row * parts + part + 1, :]
            spread = turned_product(halves(wx * wy), bq)
            for chunk, ext_ref in enumerate(ext_refs):
                ext_ref[part * step : part * step + window, row * strip : (row + 1) * strip] += (
                    spread[:, chunk * strip : (chunk + 1) * strip]
                )
    for out_ref, ext_ref in zip(out_refs, ext_refs):
        out_ref[0] = ext_ref[PAD : PAD + width]
        out_ref[0, width - PAD :] += ext_ref[:PAD]
        out_ref[0, :PAD] += ext_ref[PAD + width :]

    @pl.when(pl.program_id(0) == pl.num_programs(0) - 1)
    def _():
        for chunk, out_ref in enumerate(out_refs):
            high_ref[:, chunk * half : (chunk + 1) * half] = out_ref[0, :, :half]
            low_ref[:, chunk * half : (chunk + 1) * half] = out_ref[0, :, half : 2 * half]


def deposit_stage(weight_x, weight_y, charged, width, count):
    parts, window, slots = weight_x.shape
    groups, flat, _ = weight_y.shape
    strip = charged.shape[0] // count
    lanes = flat // parts * strip
    edge = jax.ShapeDtypeStruct((width, 2 * strip * count), jnp.float32)
    return pl.pallas_call(
        deposit_kernel,
        grid=(groups,),
        in_specs=[
            pl.BlockSpec((parts, window, slots), lambda g: (0, 0, 0)),
            pl.BlockSpec((1, flat, slots), lambda g: (g, 0, 0)),
            pl.BlockSpec(charged.shape, lambda g: (0, 0)),
        ],
        out_specs=[pl.BlockSpec((1, width, lanes), lambda g: (g, 0, 0))] * count
        + [pl.BlockSpec(edge.shape, lambda g: (0, 0))] * 2,
        out_shape=[jax.ShapeDtypeStruct((groups, width, lanes), jnp.float32)] * count + [edge] * 2,
        scratch_shapes=[pltpu.VMEM((width + 2 * PAD, lanes), jnp.float32)] * count,
        name="deposit_stage",
    )(weight_x, weight_y, charged)


def cross_kernel(chunk, parts, source_ref, *refs):
    grid_refs = refs[:parts]
    spread_ref, low_ref, high_ref, table_ref, _ = refs[parts : parts + 5]
    out_refs, block_ref = refs[parts + 5 : -1], refs[-1]
    batch, cells_x, lanes = grid_refs[0].shape
    width = table_ref.shape[0]
    strip = width // len(out_refs)
    total = batch * lanes
    half = low_ref.shape[1] // CHUNKS
    group = pl.program_id(0)
    for at in range(batch):
        for peer, grid_ref in enumerate(grid_refs):
            start = pl.multiple_of(source_ref[peer] * cells_x, 8)
            block_ref[pl.ds(start, cells_x), at * lanes : (at + 1) * lanes] = grid_ref[at]
        block_ref[:, at * lanes : (at + 1) * lanes] += spread_ref[at]

    @pl.when(group == 0)
    def _():
        block_ref[:, :half] += low_ref[:, chunk * half : (chunk + 1) * half]

    @pl.when(group == pl.num_programs(0) - 1)
    def _():
        block_ref[:, total - half :] += high_ref[:, chunk * half : (chunk + 1) * half]

    moved = product(halves(table_ref[...]), halves(block_ref[...]))
    for peer, out_ref in enumerate(out_refs):
        for at in range(batch):
            out_ref[at] = moved[
                peer * strip : (peer + 1) * strip, at * lanes : (at + 1) * lanes
            ]


def cross_stage(chunk, origin, received, spread, low, high, table, parts_y, after):
    parts = len(received)
    groups, cells_x, lanes = received[0].shape
    width = parts * cells_x
    strip = width // parts_y
    batch = 4 if groups % 4 == 0 else 1
    return pl.pallas_call(
        functools.partial(cross_kernel, chunk, parts),
        grid_spec=pltpu.PrefetchScalarGridSpec(
            num_scalar_prefetch=1,
            grid=(groups // batch,),
            in_specs=[pl.BlockSpec((batch, cells_x, lanes), lambda g, _: (g, 0, 0))] * parts
            + [
                pl.BlockSpec((batch, width, lanes), lambda g, _: (g, 0, 0)),
                pl.BlockSpec(low.shape, lambda g, _: (0, 0)),
                pl.BlockSpec(high.shape, lambda g, _: (0, 0)),
                pl.BlockSpec((width, width), lambda g, _: (0, 0)),
                pl.BlockSpec(memory_space=pl.ANY),
            ],
            out_specs=[pl.BlockSpec((batch, strip, lanes), lambda g, _: (g, 0, 0))] * parts_y,
            scratch_shapes=[pltpu.VMEM((width, batch * lanes), jnp.float32)],
        ),
        out_shape=[jax.ShapeDtypeStruct((groups, strip, lanes), jnp.float32)] * parts_y,
        name="cross_stage",
    )(origin.astype(jnp.int32), *received, spread, low, high, table, after)


def solve_kernel(parts, *refs):
    lines_refs = refs[:parts]
    ahead_ref, back_ref, square_y_ref, factor_y_ref, square_ref, factor_ref = refs[parts : parts + 6]
    out_refs, block_ref = refs[parts + 8 : -1], refs[-1]
    groups, step, lanes = lines_refs[0].shape
    beyond = out_refs[0].shape[0]
    width = ahead_ref.shape[1]
    rows = width // (parts * groups)
    strip = lanes // rows
    near = parts * groups
    far = parts * beyond
    for wave in range(step):
        held = jnp.concatenate([ref[:, wave, :] for ref in lines_refs], axis=0)
        for row in range(rows):
            block_ref[row * near : (row + 1) * near, wave * strip : (wave + 1) * strip] = held[
                :, row * strip : (row + 1) * strip
            ]
    modes = product(halves(ahead_ref[...]), halves(block_ref[...]))
    square = square_y_ref[...] + square_ref[0]
    bounded = jnp.where(square > 0.0, square, 1.0)
    green = factor_y_ref[...] * factor_ref[0] / bounded
    modes = jnp.where(square > 0.0, modes * green, 0.0)
    field = product(halves(back_ref[...]), halves(modes))
    for wave in range(step):
        held = jnp.concatenate(
            [
                field[row * far : (row + 1) * far, wave * strip : (wave + 1) * strip]
                for row in range(rows)
            ],
            axis=1,
        )
        for peer, out_ref in enumerate(out_refs):
            out_ref[:, wave, :] = held[peer * beyond : (peer + 1) * beyond]


def solve_stage(lines, ahead, back, square_y, factor_y, square, factor, after):
    parts = len(lines)
    groups, strip_x, lanes = lines[0].shape
    width = ahead.shape[0]
    extent = back.shape[0]
    beyond = groups + 1
    count = square.shape[0]
    step = strip_x // count
    waves = square.shape[-1]
    return pl.pallas_call(
        functools.partial(solve_kernel, parts),
        grid=(count,),
        in_specs=[pl.BlockSpec((groups, step, lanes), lambda g: (0, g, 0))] * parts
        + [
            pl.BlockSpec((width, width), lambda g: (0, 0)),
            pl.BlockSpec((extent, width), lambda g: (0, 0)),
            pl.BlockSpec((width, 1), lambda g: (0, 0)),
            pl.BlockSpec((width, 1), lambda g: (0, 0)),
            pl.BlockSpec((1, 1, waves), lambda g: (g, 0, 0)),
            pl.BlockSpec((1, 1, waves), lambda g: (g, 0, 0)),
            pl.BlockSpec(memory_space=pl.ANY),
            pl.BlockSpec(memory_space=pl.ANY),
        ],
        out_specs=[pl.BlockSpec((beyond, step, lanes), lambda g: (0, g, 0))] * parts,
        out_shape=[jax.ShapeDtypeStruct((beyond, strip_x, lanes), jnp.float32)] * parts,
        scratch_shapes=[pltpu.VMEM((width, waves), jnp.float32)],
        name="solve_stage",
    )(*lines, ahead, back, square_y, factor_y, square, factor, *after)


def pull_kernel(count, *refs):
    lines_refs = refs[:count]
    table_ref, wx_ref, sx_ref, wy_ref, sy_ref, bz_ref, _, out_ref, left_ref, right_ref = refs[count:]
    parts, window, slots = wx_ref.shape
    strip = bz_ref.shape[0]
    rows = wy_ref.shape[1] // parts
    width = table_ref.shape[0]
    step = width // parts
    multiply = narrow_product if rows * strip == 128 else product

    @pl.when(pl.program_id(0) == 0)
    def _():
        out_ref[...] = jnp.zeros_like(out_ref)
        for part in range(parts):
            high, low = halves(bz_ref[:, part * 2 * slots : (part + 1) * 2 * slots])
            right_ref[part] = jnp.concatenate([high, high, low], axis=0)

    block = jnp.concatenate([ref[0] for ref in lines_refs], axis=0)
    field = multiply(halves(table_ref[...]), halves(block))
    for row in range(rows):
        local = field[:, row * strip : (row + 1) * strip]
        local = jnp.concatenate([local[width - PAD :], local, local[:PAD]], axis=0)
        high, low = halves(local)
        left_ref[row] = jnp.concatenate([high, low, high], axis=1)
    for part in range(parts):
        right = right_ref[part]
        wx = wx_ref[part]
        sx = sx_ref[part]
        force_x = jnp.zeros((1, slots), jnp.float32)
        force_y = jnp.zeros((1, slots), jnp.float32)
        force_z = jnp.zeros((1, slots), jnp.float32)
        for row in range(rows):
            both = jnp.dot(
                left_ref[row, part * step : part * step + window],
                right,
                preferred_element_type=jnp.float32,
            )
            plain = both[:, :slots]
            deriv = both[:, slots:]
            at = slice(row * parts + part, row * parts + part + 1)
            wy = wy_ref[0, at, :]
            sy = sy_ref[0, at, :]
            force_x += wy * jnp.sum(sx * plain, axis=0, keepdims=True)
            force_y += sy * jnp.sum(wx * plain, axis=0, keepdims=True)
            force_z += wy * jnp.sum(wx * deriv, axis=0, keepdims=True)
        out_ref[part, 0:1] += force_x
        out_ref[part, 1:2] += force_y
        out_ref[part, 2:3] += force_z


def pull_stage(chunk, lines, table, weight_x, slope_x, weight_y, slope_y, depth_pair, after):
    parts_y = len(lines)
    groups, strip_x, lanes = lines[0].shape
    width = parts_y * strip_x
    parts, window, slots = weight_x.shape
    flat = weight_y.shape[1]
    strip = depth_pair.shape[0] // CHUNKS
    return pl.pallas_call(
        functools.partial(pull_kernel, parts_y),
        grid=(groups,),
        in_specs=[pl.BlockSpec((1, strip_x, lanes), lambda g: (g, 0, 0))] * parts_y
        + [
            pl.BlockSpec((width, width), lambda g: (0, 0)),
            pl.BlockSpec((parts, window, slots), lambda g: (0, 0, 0)),
            pl.BlockSpec((parts, window, slots), lambda g: (0, 0, 0)),
            pl.BlockSpec((1, flat, slots), lambda g: (g, 0, 0)),
            pl.BlockSpec((1, flat, slots), lambda g: (g, 0, 0)),
            pl.BlockSpec((strip, depth_pair.shape[1]), lambda g: (chunk, 0)),
            pl.BlockSpec(memory_space=pl.ANY),
        ],
        out_specs=pl.BlockSpec((parts, 8, slots), lambda g: (0, 0, 0)),
        out_shape=jax.ShapeDtypeStruct((parts, 8, slots), jnp.float32),
        scratch_shapes=[
            pltpu.VMEM((flat // parts, width + 2 * PAD, 3 * strip), jnp.bfloat16),
            pltpu.VMEM((parts, 3 * strip, 2 * slots), jnp.bfloat16),
        ],
        name="pull_stage",
    )(*lines, table, weight_x, slope_x, weight_y, slope_y, depth_pair, after)


def basis_plain(atoms, table, cells_x, cells_y, rows):
    parts, _, slots = atoms.shape
    strip, depth = table.shape
    edge_x = (jnp.arange(cells_x + 2 * PAD) - PAD).astype(jnp.float32)
    within = ((edge_x >= -2.0) & (edge_x < cells_x + 2.0))[None, :, None]
    weight_x, slope_x = (
        jnp.where(within, part, 0.0)
        for part in spline(atoms[:, 0, None, :] - edge_x[None, :, None] + 2.5)
    )
    outer = jnp.array([-2, -1, cells_y, cells_y + 1] + [-100 * cells_y] * (rows - 4))
    edge_y = jnp.concatenate([jnp.arange(cells_y), outer]).astype(jnp.float32)
    weight_y, slope_y = (
        part.reshape(cells_y // rows + 1, rows * parts, slots)
        for part in spline(atoms[None, :, 1, :] - edge_y[:, None, None] + 2.5)
    )
    halfway = depth / 2.0
    offset = atoms[None, :, 2, :] - jnp.arange(depth).astype(jnp.float32)[:, None, None]
    offset = jnp.where(offset < -halfway, offset + depth, offset)
    offset = jnp.where(offset >= halfway, offset - depth, offset)
    both = jnp.stack(spline(offset + 2.5), axis=2)
    waves = jnp.einsum("kz,zpca->kpca", table, both, precision=PRECISE)
    charged = waves[:, :, 0] * atoms[None, :, 3]
    return (
        weight_x, slope_x, weight_y, slope_y, waves.reshape(strip, -1), charged.reshape(strip, -1)
    )


def depth_plain(background, table, parts, rows, after):
    cells_y, cells_x, _ = background.shape
    moved = jnp.einsum("yxz,zk->yxk", background, table, precision=PRECISE)
    moved = moved.reshape(cells_y // rows, rows, cells_x, parts, -1).transpose(3, 0, 2, 1, 4)
    return [moved[i].reshape(cells_y // rows, cells_x, -1) for i in range(parts)]


def deposit_plain(weight_x, weight_y, charged, width, count):
    size = charged.shape[0] // count
    spreads = [
        deposit_one(weight_x, weight_y, charged[i * size : (i + 1) * size], width)
        for i in range(count)
    ]
    half = 2 * size
    low = jnp.concatenate([spread[-1, :, half : 2 * half] for spread in spreads], axis=1)
    high = jnp.concatenate([spread[-1, :, :half] for spread in spreads], axis=1)
    return spreads + [low, high]


def deposit_one(weight_x, weight_y, charged, width):
    parts, window, slots = weight_x.shape
    groups, flat, _ = weight_y.shape
    wy = weight_y.reshape(groups, flat // parts, parts, slots)
    bq = charged.reshape(-1, parts, slots)
    spread = jnp.einsum("pxa,grpa,kpa->gpxrk", weight_x, wy, bq, precision=PRECISE)
    spread = spread.reshape(groups, parts, window, -1)
    step = width // parts
    total = jnp.zeros((groups, width, spread.shape[-1]), jnp.float32)

    def add(part, total):
        place = jnp.mod(part * step - PAD + jnp.arange(window), width)
        return total.at[:, place].add(lax.dynamic_index_in_dim(spread, part, 1, False))

    return lax.fori_loop(0, parts, add, total)


def cross_plain(chunk, origin, received, spread, low, high, table, parts_y, after):
    parts = len(received)
    groups, cells_x, lanes = received[0].shape
    half = low.shape[1] // CHUNKS
    mine = slice(chunk * half, (chunk + 1) * half)
    spread = spread[:groups].at[0, :, :half].add(low[:, mine])
    spread = spread.at[groups - 1, :, lanes - half :].add(high[:, mine])
    block = jnp.stack(received, axis=1)[:, jnp.argsort(origin)]
    block = block.reshape(groups, parts * cells_x, lanes) + spread
    moved = jnp.einsum("kx,gxl->gkl", table, block, precision=PRECISE)
    moved = moved.reshape(groups, parts_y, -1, lanes)
    return [moved[:, i] for i in range(parts_y)]


def solve_plain(lines, ahead, back, square_y, factor_y, square, factor, after):
    lines = jnp.stack(lines)
    parts, groups, strip_x, lanes = lines.shape
    width = ahead.shape[0]
    rows = width // (parts * groups)
    lines = lines.reshape(parts, groups, strip_x, rows, -1).transpose(3, 0, 1, 2, 4)
    modes = jnp.dot(ahead, lines.reshape(width, -1), precision=PRECISE)
    total = square_y + square.reshape(1, -1)
    bounded = jnp.where(total > 0.0, total, 1.0)
    green = jnp.where(total > 0.0, factor_y * factor.reshape(1, -1) / bounded, 0.0)
    field = jnp.dot(back, modes * green, precision=PRECISE)
    field = field.reshape(rows, parts, groups + 1, strip_x, -1).transpose(1, 2, 3, 0, 4)
    field = field.reshape(parts, groups + 1, strip_x, lanes)
    return [field[i] for i in range(parts)]


def pull_plain(chunk, lines, table, weight_x, slope_x, weight_y, slope_y, depth_pair, after):
    lines = jnp.stack(lines)
    parts_y, groups, strip_x, lanes = lines.shape
    width = parts_y * strip_x
    parts, window, slots = weight_x.shape
    strip = depth_pair.shape[0] // CHUNKS
    pair = depth_pair[chunk * strip : (chunk + 1) * strip].reshape(strip, parts, 2 * slots)
    block = lines.transpose(1, 0, 2, 3).reshape(groups, width, lanes)
    field = jnp.einsum("xk,gkl->gxl", table, block, precision=PRECISE)
    field = field.reshape(groups, width, lanes // strip, strip)
    step = width // parts
    wy = weight_y.reshape(groups, -1, parts, slots)
    sy = slope_y.reshape(groups, -1, parts, slots)

    def one(part):
        take = functools.partial(lax.dynamic_index_in_dim, index=part, keepdims=False)
        place = jnp.mod(part * step - PAD + jnp.arange(window), width)
        both = jnp.einsum("gxrk,ka->gxra", field[:, place], take(pair, axis=1), precision=PRECISE)
        plain = both[..., :slots]
        deriv = both[..., slots:]
        wx = take(weight_x, axis=0)[None, :, None, :]
        sx = take(slope_x, axis=0)[None, :, None, :]
        up = take(wy, axis=2)
        return jnp.stack(
            [
                jnp.sum(up * jnp.sum(sx * plain, axis=1), axis=(0, 1)),
                jnp.sum(take(sy, axis=2) * jnp.sum(wx * plain, axis=1), axis=(0, 1)),
                jnp.sum(up * jnp.sum(wx * deriv, axis=1), axis=(0, 1)),
            ]
        )

    out = lax.map(one, jnp.arange(parts))
    return jnp.pad(out, ((0, 0), (0, 5), (0, 0)))


def ring(axis, step):
    count = lax.axis_size(axis)
    return [(i, (i + step) % count) for i in range(count)]


CHUNKS = 3


def partner(index, step, count):
    if count & (count - 1) == 0:
        return index ^ step, index ^ step
    return (index + step) % count, (index - step) % count


def targets(index, count):
    return jnp.stack([partner(index, step, count)[0] for step in range(count)])


def sources(index, count):
    return jnp.stack([partner(index, step, count)[1] for step in range(count)])


def exchange(blocks, axis):
    count = len(blocks)
    got = [blocks[0]]
    for step in range(1, count):
        pairs = [(i, partner(i, step, count)[0]) for i in range(count)]
        got.append(lax.ppermute(blocks[step], axis, pairs))
    return got


def device_forces(atom_x, atom_y, atom_z, charges, counts, background):
    slots = atom_x.shape[-1]
    cells_y, cells_x, depth = background.shape
    parts_x = lax.axis_size("gx")
    parts_y = lax.axis_size(PLANE)
    width_x = cells_x * parts_x
    width_y = cells_y * parts_y
    strip_z = depth // parts_x
    strip_x = width_x // parts_y
    part_z = strip_z // CHUNKS
    tiled = 4 * part_z % 128 == 0 and cells_x % 8 == 0 and strip_x % 8 == 0 and cells_y % 4 == 0
    rows = 4 if tiled else cells_y
    groups = cells_y // rows
    if tiled:
        basis_do, depth_do, deposit_do, cross_do, solve_do, pull_do = (
            basis_stage, depth_stage, deposit_stage, cross_stage, solve_stage, pull_stage
        )
    else:
        basis_do, depth_do, deposit_do, cross_do, solve_do, pull_do = (
            basis_plain, depth_plain, deposit_plain, cross_plain, solve_plain, pull_plain
        )
    place_x = lax.axis_index("gx")
    place_y = lax.axis_index(PLANE)

    live = jnp.arange(slots) < counts.reshape(())
    charge_live = jnp.where(live, charges.reshape(slots), 0.0)
    own = jnp.stack(
        [atom_x.reshape(slots), atom_y.reshape(slots), atom_z.reshape(slots), charge_live]
    )
    gathered = exchange([own] * parts_x, "gx")

    starts = targets(place_x, parts_x)[:, None] * strip_z + jnp.arange(part_z)

    def first_pass(chunk, after):
        table = cas_table(jnp.arange(depth), (starts + chunk * part_z).reshape(-1), depth)
        return depth_do(background, table, parts_x, rows, after)

    sent = first_pass(0, atom_x)
    received = [exchange(sent, "gx")]
    for i in range(1, CHUNKS - 1):
        sent = first_pass(i, sent[0])
        received.append(exchange(sent, "gx"))
    origin = sources(place_x, parts_x)
    turned = sources(place_x, parts_x) if parts_x & (parts_x - 1) == 0 else jnp.mod(
        place_x - jnp.arange(parts_x), parts_x
    )
    gathered = jnp.stack(gathered)
    atoms = jnp.stack(
        [lax.dynamic_index_in_dim(gathered, turned[i], 0, False) for i in range(parts_x)]
    )

    modes_z = place_x * strip_z + jnp.arange(strip_z)
    modes_x = place_y * strip_x + jnp.arange(strip_x)
    cells_all = jnp.arange(width_x)
    strips = jnp.arange(strip_x)
    sent_x = (targets(place_y, parts_y)[:, None] * strip_x + strips).reshape(-1)
    came_x = (sources(place_y, parts_y)[:, None] * strip_x + strips).reshape(-1)
    table_x = cas_table(sent_x, cells_all, width_x)
    table_back_x = cas_table(cells_all, came_x, width_x)
    table_strip = cas_table(modes_z, jnp.arange(depth), depth)
    weight_x, slope_x, weight_y, slope_y, depth_pair, charged = basis_do(
        atoms, table_strip, cells_x, cells_y, rows
    )
    *spreads, low, high = deposit_do(weight_x, weight_y, charged, width_x, CHUNKS)
    low = lax.ppermute(low, PLANE, ring(PLANE, 1))
    high = lax.ppermute(high, PLANE, ring(PLANE, -1))

    def cross_of(i, after):
        return cross_do(
            i, origin, received[i], spreads[i], low, high, table_x, parts_y, after
        )

    columns = cross_of(0, low)
    lines = [exchange(columns, PLANE)]
    received.append(exchange(first_pass(CHUNKS - 1, columns[0]), "gx"))
    place_y, modes_y, _ = lax.optimization_barrier((place_y, jnp.arange(width_y), columns[0]))
    inner = jnp.arange(cells_y)
    outer = jnp.array([-2, -1, cells_y, cells_y + 1] + [-100 * cells_y] * (rows - 4))

    near = (
        jnp.arange(rows)[:, None, None]
        + sources(place_y, parts_y)[None, :, None] * cells_y
        + jnp.arange(groups)[None, None, :] * rows
    )
    sent_y = (
        jnp.arange(rows)[:, None, None]
        + targets(place_y, parts_y)[None, :, None] * cells_y
        + jnp.arange(groups)[None, None, :] * rows
    )
    far = jnp.broadcast_to(
        jnp.where(outer < -cells_y, 0, outer)[:, None, None]
        + targets(place_y, parts_y)[None, :, None] * cells_y,
        (rows, parts_y, 1),
    )
    ahead = cas_table(modes_y, near.reshape(-1), width_y)
    cells = jnp.mod(jnp.concatenate([sent_y, far], axis=2).reshape(-1), width_y)
    back = cas_table(cells, modes_y, width_y)
    square_y, factor_y = axis_factors(modes_y, width_y)
    square_x, factor_x = axis_factors(modes_x, width_x)
    square_z, factor_z = axis_factors(modes_z, depth)
    scale = COULOMB / (math.pi * width_x * width_y * depth)
    step = 8 if tiled else strip_x

    def solve_of(i, after):
        at = slice(i * part_z, (i + 1) * part_z)
        square = (square_x[:, None] + square_z[None, at]).reshape(strip_x // step, 1, -1)
        factor = (scale * factor_x[:, None] * factor_z[None, at]).reshape(square.shape)
        return solve_do(
            lines[i], ahead, back, square_y[:, None], factor_y[:, None], square, factor, after
        )

    def pull_of(i, after):
        return pull_do(
            i, returned[i], table_back_x, weight_x, slope_x, weight_y, slope_y, depth_pair,
            after,
        )

    columns = cross_of(1, columns[0])
    lines.append(exchange(columns, PLANE))
    solved = solve_of(0, (columns[0], columns[0]))
    returned = [exchange(solved, PLANE)]
    for i in range(2, CHUNKS):
        columns = cross_of(i, solved[0])
        lines.append(exchange(columns, PLANE))
    solved = solve_of(1, (columns[0], columns[0]))
    returned.append(exchange(solved, PLANE))
    partial = pull_of(0, solved[0])
    for i in range(2, CHUNKS):
        solved = solve_of(i, (solved[0], solved[0]))
        returned.append(exchange(solved, PLANE))
    for i in range(1, CHUNKS):
        partial += pull_of(i, solved[0])
    goal = targets(place_x, parts_x)
    blocks = [lax.dynamic_index_in_dim(partial, goal[i], 0, False) for i in range(parts_x)]
    forces = -charge_live * sum(exchange(blocks, "gx"))[:3]
    return forces.reshape(3, 1, 1, slots)


def solution(mesh):
    in_specs = (
        P("gx", PLANE, None),
        P("gx", PLANE, None),
        P("gx", PLANE, None),
        P("gx", PLANE, None),
        P("gx", PLANE),
        P(PLANE, "gx", None),
    )
    out_specs = P(None, "gx", PLANE, None)
    return jax.shard_map(
        device_forces,
        mesh=mesh,
        in_specs=in_specs,
        out_specs=out_specs,
        check_vma=False,
    )
```
